128 devices in a mesh: seq: 16 (over x, z), head: 4 (over y), batch: 2 (over core).
Axes of the slice: x: 4, y: 4, z: 4, core: 2. Of those that a mesh axis runs over, the one named last changes fastest.
Arguments:
- queries: bfloat16 [2, 8192, 32, 128], P('batch', 'seq', 'head'), may hold values from -200 to 200
- key_states: bfloat16 [2, 8192, 8, 128], P('batch', 'seq', 'head'), may hold values from -7 to 7
- value_vectors: bfloat16 [2, 8192, 8, 128], P('batch', 'seq', 'head'), may hold values from -6 to 6
- block_doc: int32 [2, 64], P('batch'), may hold values from 0 to 15, never falling along the last dimension, each value on 1 to 36 neighbouring positions
- out_weight: bfloat16 [4096, 8192], P('head', 'batch'), may hold values from -0.5 to 0.5
Outputs:
- projected: bfloat16 [8192, 2, 8192], P(('seq', 'head'), None, 'batch')
The draws below stay inside these ranges and needn't reach their ends.
Inputs may be any that keep to these rules, and one draw needn't show every extreme that they name: block_doc[b, j] never falls along j, starts at 0 and skips no number; every document covers 1 to 36 whole blocks, and some document covers exactly 36.
All inputs are finite; a program needn't handle non-finite values.
Results may differ from the reference program's by a relative error of at most 0.0095.
Values may be sent and summed in bfloat16 or wider, within the bound.
No kernel may reach another device: no remote copies, remote signals or barrier semaphores. Data moves between devices by JAX's collectives and lax.ppermute only.
A program may use at most 128 MiB of HBM per device.

```python
import math
import jax
import jax.numpy as jnp
import numpy as np
from jax import lax

D = 8192
QUERY_HEADS = 32
KEY_VALUE_HEADS = 8
HEAD_WIDTH = 128
BLK = 128
SEQUENCE_LENGTH = 8192
PACKED_BATCH = 2
NBLK = 64
MOSTB = 36
NDOC = 16
HQ_DEV = 8
HGROUPS = 4


def draw_pair(key):
    query_draw = jax.random.normal(jax.random.fold_in(key, 11), (PACKED_BATCH, SEQUENCE_LENGTH, QUERY_HEADS, HEAD_WIDTH), jnp.float32)
    key_sample = jnp.clip(jax.random.normal(jax.random.fold_in(key, 12), (PACKED_BATCH, SEQUENCE_LENGTH, KEY_VALUE_HEADS, HEAD_WIDTH), jnp.float32), -6.0, 6.0)
    query_draw = jnp.clip(query_draw, -6.0, 6.0)
    return (query_draw, key_sample)


def draw_queries(key, part):
    return draw_pair(key)[0].astype(jnp.bfloat16)


def draw_key_states(key, part):
    return draw_pair(key)[1].astype(jnp.bfloat16)


def shard_levels(stream_key, extent, cuts, low, top_value):
    loudness, own = 1.0, jax.random.fold_in(stream_key, 6)
    for dim, blocks in cuts:
        heights = jnp.exp(jax.random.uniform(jax.random.fold_in(own, dim), (blocks,), jnp.float32, low / len(cuts), top_value / len(cuts)))
        loudness = loudness * jnp.repeat(heights, extent[dim] // blocks).reshape([-1 if axis == dim else 1 for axis in range(len(extent))])
    return loudness


def profile(count, total, limit, slope):
    weights = [(1 << 20) // math.isqrt(grade ** slope) + 1 for grade in range(2, count + 1)]
    rest, given = total - limit - (count - 1), [1] * (count - 1)
    while rest > 0:
        free = [i for i in range(count - 1) if given[i] < limit]
        pool, budget = sum([weights[i] for i in free]), rest
        for i in free:
            addition = min(limit - given[i], max(1, budget * weights[i] // pool), rest)
            given[i] = given[i] + addition
            rest = rest - addition
    return np.array([limit] + given)


def ragged_sizes(key, amount, total, limit, lean):
    if amount == 2:
        one = jax.random.randint(key, (), max(1, total - limit), min(limit, total - 1) + 1)
        return jnp.stack([one, total - one])
    tallies = jnp.asarray(profile(amount, total, limit, lean), jnp.int32)
    pairs = (amount - 1) // 2
    source_of, receiver = tallies[1:1 + 2 * pairs:2], tallies[2:2 + 2 * pairs:2]
    slack = jnp.minimum(source_of - 1, limit - receiver)
    moved = jax.random.randint(jax.random.fold_in(key, 1), (pairs,), 0, 1 << 20) % (slack + 1)
    tallies = tallies.at[1:1 + 2 * pairs:2].set(source_of - moved).at[2:2 + 2 * pairs:2].set(receiver + moved)
    return tallies[jax.random.permutation(jax.random.fold_in(key, 2), amount)]


def gaussian(key, shape, spread, most, split=(), kind=jnp.bfloat16):
    drawn = spread * jax.random.normal(key, shape, jnp.float32)
    if split:
        drawn = drawn * shard_levels(key, shape, split, -0.22, 0.18)
    return jnp.clip(drawn, -most, most).astype(kind)


def setup_inputs(seed: int = 0) -> dict:
    streams_of = jax.random.split(jax.random.key(seed), 6)
    queries = draw_queries(jax.random.fold_in(streams_of[5], 71), 0)
    key_states = draw_key_states(jax.random.fold_in(streams_of[5], 71), 0)
    value_vectors = gaussian(streams_of[2], (PACKED_BATCH, SEQUENCE_LENGTH, KEY_VALUE_HEADS, HEAD_WIDTH), 1.0, 6.0, ((0, 2), (1, 16), (2, 4)))
    block_doc = jax.vmap(lambda own: jnp.searchsorted(jnp.cumsum(ragged_sizes(own, NDOC, NBLK, MOSTB, 2)), jnp.arange(NBLK), side="right"))(jax.random.split(streams_of[3], PACKED_BATCH)).reshape((PACKED_BATCH, NBLK)).astype(jnp.int32)
    out_weight = gaussian(streams_of[4], (QUERY_HEADS * HEAD_WIDTH, D), HEAD_WIDTH ** -0.5, 0.5, ((0, 4), (1, 2)))
    return {"queries": queries, "key_states": key_states, "value_vectors": value_vectors, "block_doc": block_doc, "out_weight": out_weight}


def reference(queries, key_states, value_vectors, block_doc, out_weight):
    group_count_per_key = QUERY_HEADS // KEY_VALUE_HEADS
    score_scale = HEAD_WIDTH ** -0.5
    positions = jnp.arange(SEQUENCE_LENGTH, dtype=jnp.int32)
    results = []
    for batch_index in range(PACKED_BATCH):
        doc_tok = jnp.repeat(block_doc[batch_index], BLK)
        visible = (doc_tok[:, None] == doc_tok[None, :]) & (positions[:, None] >= positions[None, :])
        query_seq = queries[batch_index]
        key_seq = key_states[batch_index]
        value_seq = value_vectors[batch_index]

        def head_out(head_index):
            q_head = lax.dynamic_index_in_dim(query_seq, head_index, 1, False)
            k_head = lax.dynamic_index_in_dim(key_seq, head_index // group_count_per_key, 1, False)
            v_head = lax.dynamic_index_in_dim(value_seq, head_index // group_count_per_key, 1, False)
            scores = jnp.dot(q_head, k_head.T, preferred_element_type=jnp.float32) * score_scale
            scores = jnp.where(visible, scores, -1e30)
            maxima = jnp.max(scores, axis=1)
            weights = jnp.where(visible, jnp.exp(scores - maxima[:, None]), 0.0)
            denominator = jnp.sum(weights, axis=1)
            numerator = jnp.dot(weights.astype(jnp.bfloat16), v_head, preferred_element_type=jnp.float32)
            return (numerator / denominator[:, None]).astype(jnp.bfloat16)

        attended = lax.map(head_out, jnp.arange(QUERY_HEADS, dtype=jnp.int32))
        flattened = jnp.transpose(attended, (1, 0, 2)).reshape(SEQUENCE_LENGTH, QUERY_HEADS * HEAD_WIDTH)
        group_width = HQ_DEV * HEAD_WIDTH
        summed = jnp.zeros((SEQUENCE_LENGTH, D), jnp.float32)
        for group_index in range(HGROUPS):
            lower = group_index * group_width
            partial_value = jnp.dot(flattened[:, lower:lower + group_width], out_weight[lower:lower + group_width], preferred_element_type=jnp.float32).astype(jnp.bfloat16)
            partial_value = lax.optimization_barrier(partial_value)
            summed = summed + partial_value.astype(jnp.float32)
        results.append(summed.astype(jnp.bfloat16))
    return jnp.stack(results, axis=1)
```

```python
import math

import jax
import jax.numpy as jnp
from jax import lax
from jax.experimental import pallas as pl
from jax.experimental.pallas import tpu as pltpu
from jax.sharding import PartitionSpec as P


XN = 4
ZN = 4
TOK = 512
BLK = 128
HD = 128
GRP = 4
BPD = TOK // BLK
REACH = 9
SLOTS = REACH + 1
SCALE = math.log2(math.e) / math.sqrt(HD)
NEG = -1e30


UNITS = tuple(
    (g, dz, part)
    for g in range(3)
    for dz, part in ((0, 2), (-1, 2), (1, 2), (2, 0), (2, 1))
) + ((3, 3, 2),)


def attn_kernel(doc_ref, q_ref, *refs):
    n = len(UNITS)
    unit_refs = refs[:n]
    o_ref = refs[n]
    kv, m_ref, l_ref, acc_ref, sems = refs[n + 1 :]
    s_idx = lax.axis_index("seq")
    x_idx = s_idx // ZN
    z_idx = s_idx % ZN
    first_doc = doc_ref[0, BPD * s_idx]

    copies = []
    for i, (g, dz, part) in enumerate(UNITS):
        src = ZN * (x_idx - g) + (z_idx + dz + ZN) % ZN
        delta = s_idx - src
        safe = jnp.maximum(src, 0)
        need = (
            (src >= 0)
            & (delta >= 0)
            & (delta <= REACH)
            & ((g < 3) | (z_idx == 0))
            & (doc_ref[0, BPD * safe + BPD - 1] >= first_doc)
        )
        slot = jnp.clip(delta, 0, REACH)
        if part == 2:
            dst = kv.at[slot]
        else:
            dst = kv.at[slot, part]
        copy = pltpu.make_async_copy(unit_refs[i], dst, sems.at[i])
        copies.append((need, copy))
    for need, copy in copies:
        pl.when(need)(copy.start)
    for need, copy in copies:
        pl.when(need)(copy.wait)

    def tile(j, slot, mask):
        for h in range(GRP):
            q = q_ref[pl.ds(pl.multiple_of(j * BLK, BLK), BLK), h * HD : (h + 1) * HD]
            s = lax.dot_general(
                q, kv[slot, 0], (((1,), (1,)), ((), ())), preferred_element_type=jnp.float32
            )
            if mask is not None:
                s = jnp.where(mask, s, NEG)
            m_prev = m_ref[h]
            m_new = jnp.maximum(m_prev, jnp.max(s, axis=1, keepdims=True))
            m_wide = jnp.concatenate([m_new] * (TOK // HD), axis=1)
            p = jnp.exp2((s - m_wide) * SCALE)
            alpha = jnp.exp2((m_prev - m_new) * SCALE)
            part_sum = p[:, 0:HD]
            for c in range(1, TOK // HD):
                part_sum = part_sum + p[:, c * HD : (c + 1) * HD]
            l_ref[h] = l_ref[h] * alpha + part_sum
            pv = jnp.dot(p.astype(jnp.bfloat16), kv[slot, 1], preferred_element_type=jnp.float32)
            acc_ref[h] = acc_ref[h] * alpha + pv
            m_ref[h] = m_new

    def doc_mask(src, doc_q):
        hidden = jnp.int32(0)
        for b in range(BPD - 1):
            hidden = hidden + (doc_ref[0, BPD * src + b] != doc_q).astype(jnp.int32)
        key_pos = lax.broadcasted_iota(jnp.int32, (BLK, TOK), 1)
        return key_pos, key_pos >= hidden * BLK

    @pl.loop(0, BPD)
    def _(j):
        m_ref[...] = jnp.full_like(m_ref, NEG)
        l_ref[...] = jnp.zeros_like(l_ref)
        acc_ref[...] = jnp.zeros_like(acc_ref)
        doc_q = doc_ref[0, BPD * s_idx + j]
        full = jnp.int32(0)
        some = jnp.int32(0)
        for d in range(1, REACH + 1):
            src = s_idx - d
            safe = jnp.maximum(src, 0)
            valid = src >= 0
            full = full + (valid & (doc_ref[0, BPD * safe] == doc_q)).astype(jnp.int32)
            some = some + (valid & (doc_ref[0, BPD * safe + BPD - 1] == doc_q)).astype(jnp.int32)
        hidden = jnp.int32(0)
        for b in range(BPD - 1):
            hidden = hidden + (doc_ref[0, BPD * s_idx + b] < doc_q).astype(jnp.int32)
        key_pos = lax.broadcasted_iota(jnp.int32, (BLK, TOK), 1)
        row_pos = lax.broadcasted_iota(jnp.int32, (BLK, TOK), 0) + j * BLK
        tile(j, 0, (key_pos <= row_pos) & (key_pos >= hidden * BLK))

        @pl.loop(1, full + 1)
        def _(d):
            tile(j, d, None)

        @pl.when(some > full)
        def _():
            d = jnp.minimum(full + 1, REACH)
            _, mask = doc_mask(jnp.maximum(s_idx - d, 0), doc_q)
            tile(j, d, mask)

        for h in range(GRP):
            total = jnp.sum(l_ref[h], axis=1, keepdims=True)
            o_ref[pl.ds(pl.multiple_of(j * BLK, BLK), BLK), h * HD : (h + 1) * HD] = (
                acc_ref[h] / total
            ).astype(o_ref.dtype)


def attention(doc, q, units):
    n = len(UNITS)
    return pl.pallas_call(
        attn_kernel,
        name="attend",
        out_shape=jax.ShapeDtypeStruct((TOK, GRP * HD), jnp.bfloat16),
        in_specs=[
            pl.BlockSpec(memory_space=pltpu.SMEM),
            pl.BlockSpec(memory_space=pltpu.VMEM),
        ]
        + [pl.BlockSpec(memory_space=pl.ANY)] * n,
        out_specs=pl.BlockSpec(memory_space=pltpu.VMEM),
        scratch_shapes=[
            pltpu.VMEM((SLOTS, 2, TOK, HD), jnp.bfloat16),
            pltpu.VMEM((GRP, BLK, HD), jnp.float32),
            pltpu.VMEM((GRP, BLK, HD), jnp.float32),
            pltpu.VMEM((GRP, BLK, HD), jnp.float32),
            pltpu.SemaphoreType.DMA((n,)),
        ],
        compiler_params=pltpu.CompilerParams(vmem_limit_bytes=16 << 20),
        cost_estimate=pl.CostEstimate(
            flops=6_000_000_000, bytes_accessed=4_000_000, transcendentals=8_000_000
        ),
    )(doc, q, *units)


def along_z(v, step, first_row):
    pairs = [
        (ZN * x + z, ZN * x + (z + step) % ZN) for x in range(first_row, XN) for z in range(ZN)
    ]
    return lax.ppermute(v, "seq", pairs)


def along_x(v, first_row):
    pairs = [(ZN * x + z, ZN * (x + 1) + z) for x in range(first_row, XN - 1) for z in range(ZN)]
    return lax.ppermute(v, "seq", pairs)


def gather_units(own):
    x1 = along_x(own, 0)
    x2 = along_x(x1, 1)
    units = []
    for row, group in enumerate((own, x1, x2)):
        below = along_z(group, 1, row)
        above = along_z(group, -1, row)
        far_k = along_z(below[0], 1, row)
        far_v = along_z(above[1], -1, row)
        units += [group, below, above, far_k, far_v]
    units.append(lax.ppermute(own, "seq", [(ZN - 1, ZN * (XN - 1))]))
    return units


def add_kernel(idx_ref, ra_ref, rb_ref, pa_ref, pb_ref, na_ref, nb_ref):
    na_ref[...] = ra_ref[...] + pa_ref[...]
    nb_ref[...] = rb_ref[...] + pb_ref[...]


def ring_add(idx, turn, ra, rb, partial):
    rows, half = ra.shape
    tile = half // 2
    nt = half // tile
    return pl.pallas_call(
        add_kernel,
        name="ring_add",
        out_shape=[jax.ShapeDtypeStruct(ra.shape, ra.dtype)] * 2,
        grid_spec=pltpu.PrefetchScalarGridSpec(
            num_scalar_prefetch=1,
            grid=(nt,),
            in_specs=[
                pl.BlockSpec((rows, tile), lambda i, idx: (0, i)),
                pl.BlockSpec((rows, tile), lambda i, idx: (0, i)),
                pl.BlockSpec((rows, tile), lambda i, idx: (idx[2 * turn], i)),
                pl.BlockSpec((rows, tile), lambda i, idx: (idx[2 * turn + 1], nt + i)),
            ],
            out_specs=[
                pl.BlockSpec((rows, tile), lambda i, idx: (0, i)),
                pl.BlockSpec((rows, tile), lambda i, idx: (0, i)),
            ],
        ),
        cost_estimate=pl.CostEstimate(
            flops=1_000_000, bytes_accessed=6 * rows * half * 2, transcendentals=0
        ),
    )(idx, ra, rb, partial, partial)


def around(v, step):
    n = lax.axis_size("head")
    return lax.ppermute(v, "head", [(i, (i + step) % n) for i in range(n)])


def ring_sum(idx, partial):
    me = lax.axis_index("head")
    n = lax.axis_size("head")
    rows = partial.shape[0] // n
    half = partial.shape[1] // 2
    a = lax.dynamic_slice(partial, ((me + n - 1) % n * rows, 0), (rows, half))
    b = lax.dynamic_slice(partial, ((me + 1) % n * rows, half), (rows, half))
    for turn in range(n - 1):
        a, b = around(a, 1), around(b, -1)
        a, b = ring_add(idx, turn, a, b, partial)
    return jnp.concatenate([a, b], axis=1)


def swapped(v):
    return lax.ppermute(v, "batch", [(0, 1), (1, 0)])


def on_device(queries, key_states, value_vectors, block_doc, out_weight):
    core = lax.axis_index("batch")
    first = core == 0
    q2 = queries[0].reshape(TOK, 2 * GRP * HD)
    halves_q = (q2[:, : GRP * HD], q2[:, GRP * HD :])
    halves_kv = tuple(
        jnp.stack([key_states[0, :, h], value_vectors[0, :, h]], axis=0) for h in range(2)
    )
    kv_mine = jnp.where(first, halves_kv[0], halves_kv[1])
    kv_theirs = swapped(jnp.where(first, halves_kv[1], halves_kv[0]))
    q_mine = jnp.where(first, halves_q[0], halves_q[1])
    q_theirs = swapped(jnp.where(first, halves_q[1], halves_q[0]))
    doc_theirs = swapped(block_doc)

    def of(sequence, mine, theirs):
        return jnp.where(core == sequence, mine, theirs)

    n = lax.axis_size("head")
    me = lax.axis_index("head")
    idx = jnp.stack([(me + d) % n for t in range(n - 1) for d in (2 * n - 2 - t, 2 + t)])

    results = []
    for sequence in range(2):
        units = gather_units(of(sequence, kv_mine, kv_theirs))
        attended = attention(
            of(sequence, block_doc, doc_theirs), of(sequence, q_mine, q_theirs), units
        )
        other = swapped(attended)
        both = jnp.where(
            first,
            jnp.concatenate([attended, other], axis=1),
            jnp.concatenate([other, attended], axis=1),
        )
        partial = jnp.dot(both, out_weight, preferred_element_type=jnp.float32).astype(
            jnp.bfloat16
        )
        results.append(ring_sum(idx, partial))
    return jnp.stack(results, axis=1)


def solution(mesh):
    return jax.shard_map(
        on_device,
        mesh=mesh,
        in_specs=(
            P("batch", "seq", "head", None),
            P("batch", "seq", "head", None),
            P("batch", "seq", "head", None),
            P("batch", None),
            P("head", "batch"),
        ),
        out_specs=P(("seq", "head"), None, "batch"),
        check_vma=False,
    )
```

```python
import functools
import math

import jax
import jax.numpy as jnp
from jax import lax
from jax.experimental import pallas as pl
from jax.experimental.pallas import tpu as pltpu
from jax.sharding import PartitionSpec as P


XN = 4
ZN = 4
TOK = 512
BLK = 128
HD = 128
GRP = 4
BPD = TOK // BLK
REACH = 9
SLOTS = REACH + 1
SCALE = math.log2(math.e) / math.sqrt(HD)
NEG = -1e30


NAMES = (
    "own",
    "x1",
    "x2",
    "below_own",
    "below_x1",
    "below_x2",
    "above_mixed",
    "above_x1",
    "far_mixed",
    "far_x1",
    "corner",
)


def unit_source(name, x, z):
    below, above, far = (z + ZN - 1) % ZN, (z + 1) % ZN, (z + 2) % ZN
    at = {
        "own": (x, z),
        "x1": (x - 1, z),
        "x2": (x - 2, z),
        "below_own": (x, below),
        "below_x1": (x - 1, below),
        "below_x2": (x - 2, below),
        "above_mixed": (jnp.where(z == ZN - 1, x, x - 2), above),
        "above_x1": (x - 1, above),
        "far_mixed": (jnp.where(z >= 2, x, x - 2), far),
        "far_x1": (x - 1, far),
        "corner": (jnp.where(z == 0, x - 3, -1), ZN - 1),
    }[name]
    return ZN * at[0] + at[1]


APART = tuple((i, None) for i in range(len(NAMES)))
STACKED = (
    (0, 0),
    (0, 1),
    (0, 2),
    (1, 0),
    (1, 1),
    (1, 2),
    (2, 0),
    (2, 1),
    (3, None),
    (4, None),
    (5, None),
)


def attn_kernel(spec, n, span, doc_ref, q_ref, *refs):
    unit_refs = refs[:n]
    o_ref = refs[n]
    kv, qs, m_ref, l_ref, acc_ref, s_a, s_b, p_a, p_b, a_a, a_b, sems = refs[n + 1 :]
    s_idx = lax.axis_index("seq")
    x_idx = s_idx // ZN
    z_idx = s_idx % ZN
    first_doc = doc_ref[0, BPD * s_idx]

    copies = []
    for i, (operand, at) in enumerate(spec):
        src = unit_source(NAMES[i], x_idx, z_idx)
        delta = s_idx - src
        safe = jnp.maximum(src, 0)
        need = (
            (src >= 0)
            & (delta >= 0)
            & (delta <= REACH)
            & (doc_ref[0, BPD * safe + BPD - 1] >= first_doc)
        )
        slot = jnp.clip(delta, 0, REACH)
        unit = unit_refs[operand]
        if at is not None:
            unit = unit.at[at]
        copy = pltpu.make_async_copy(unit, kv.at[slot], sems.at[i])
        copies.append((need, copy))
    for need, copy in copies:
        pl.when(need)(copy.start)
    for need, copy in copies:
        pl.when(need)(copy.wait)

    def score(dst, slot, mask=None):
        s = lax.dot_general(
            qs[...], kv[slot, 0], (((1,), (1,)), ((), ())), preferred_element_type=jnp.float32
        )
        if mask is None:
            dst[...] = s
        else:
            for h in range(GRP):
                rows = slice(h * BLK, (h + 1) * BLK)
                dst[rows] = jnp.where(mask, s[rows], NEG)

    def soften(src, p_dst, a_dst):
        for h in range(GRP):
            rows = slice(h * BLK, (h + 1) * BLK)
            sh = src[rows]
            m_prev = m_ref[rows]
            m_new = jnp.maximum(m_prev, jnp.max(sh, axis=1, keepdims=True))
            m_wide = jnp.concatenate([m_new] * (TOK // HD), axis=1)
            p = jnp.exp2((sh - m_wide) * SCALE)
            alpha = jnp.exp2((m_prev - m_new) * SCALE)
            part_sum = p[:, 0:HD]
            for c in range(1, TOK // HD):
                part_sum = part_sum + p[:, c * HD : (c + 1) * HD]
            l_ref[rows] = l_ref[rows] * alpha + part_sum
            m_ref[rows] = m_new
            a_dst[rows] = alpha
            p_dst[rows] = p.astype(jnp.bfloat16)

    def mix(p_src, a_src, slot):
        pv = jnp.dot(p_src[...], kv[slot, 1], preferred_element_type=jnp.float32)
        acc_ref[...] = acc_ref[...] * a_src[...] + pv

    @pl.loop(span[0], span[1])
    def _(j):
        for h in range(GRP):
            qs[h * BLK : (h + 1) * BLK] = q_ref[
                pl.ds(pl.multiple_of(j * BLK, BLK), BLK), h * HD : (h + 1) * HD
            ]
        m_ref[...] = jnp.full_like(m_ref, NEG)
        l_ref[...] = jnp.zeros_like(l_ref)
        acc_ref[...] = jnp.zeros_like(acc_ref)
        doc_q = doc_ref[0, BPD * s_idx + j]
        full = jnp.int32(0)
        some = jnp.int32(0)
        for d in range(1, REACH + 1):
            src = s_idx - d
            safe = jnp.maximum(src, 0)
            valid = src >= 0
            full = full + (valid & (doc_ref[0, BPD * safe] == doc_q)).astype(jnp.int32)
            some = some + (valid & (doc_ref[0, BPD * safe + BPD - 1] == doc_q)).astype(jnp.int32)
        key_pos = lax.broadcasted_iota(jnp.int32, (BLK, TOK), 1)
        row_pos = lax.broadcasted_iota(jnp.int32, (BLK, TOK), 0) + j * BLK

        def hidden_keys(unit):
            hidden = jnp.int32(0)
            for b in range(BPD - 1):
                hidden = hidden + (doc_ref[0, BPD * unit + b] < doc_q).astype(jnp.int32)
            return hidden * BLK

        score(s_b, 0, (key_pos <= row_pos) & (key_pos >= hidden_keys(s_idx)))
        soften(s_b, p_b, a_b)

        edge = jnp.minimum(full + 1, REACH)

        @pl.when(some > full)
        def _():
            score(s_a, edge, key_pos >= hidden_keys(jnp.maximum(s_idx - edge, 0)))
            mix(p_b, a_b, 0)
            soften(s_a, p_b, a_b)

        pend = jnp.where(some > full, edge, 0)
        odd = full % 2

        @pl.when(odd == 1)
        def _():
            score(s_a, 1)
            mix(p_b, a_b, pend)
            soften(s_a, p_b, a_b)

        pend = jnp.where(odd == 1, 1, pend)

        @pl.when(full > 1)
        def _():
            score(s_a, 1 + odd)

        @pl.loop(0, full // 2)
        def _(i):
            t = 1 + odd + 2 * i
            score(s_b, t + 1)
            soften(s_a, p_a, a_a)
            mix(p_b, a_b, jnp.where(i == 0, pend, t - 1))
            score(s_a, jnp.minimum(t + 2, full))
            soften(s_b, p_b, a_b)
            mix(p_a, a_a, t)

        mix(p_b, a_b, jnp.where(full > 1, full, pend))

        for h in range(GRP):
            rows = slice(h * BLK, (h + 1) * BLK)
            total = jnp.sum(l_ref[rows], axis=1, keepdims=True)
            o_ref[pl.ds(pl.multiple_of((j - span[0]) * BLK, BLK), BLK), h * HD : (h + 1) * HD] = (
                acc_ref[rows] / total
            ).astype(o_ref.dtype)


def attention(doc, q, units, spec, span):
    n = len(units)
    return pl.pallas_call(
        functools.partial(attn_kernel, spec, n, span),
        name="attend",
        out_shape=jax.ShapeDtypeStruct(((span[1] - span[0]) * BLK, GRP * HD), jnp.bfloat16),
        in_specs=[
            pl.BlockSpec(memory_space=pltpu.SMEM),
            pl.BlockSpec(memory_space=pltpu.VMEM),
        ]
        + [pl.BlockSpec(memory_space=pl.ANY)] * n,
        out_specs=pl.BlockSpec(memory_space=pltpu.VMEM),
        scratch_shapes=[
            pltpu.VMEM((SLOTS, 2, TOK, HD), jnp.bfloat16),
            pltpu.VMEM((GRP * BLK, HD), jnp.bfloat16),
            pltpu.VMEM((GRP * BLK, HD), jnp.float32),
            pltpu.VMEM((GRP * BLK, HD), jnp.float32),
            pltpu.VMEM((GRP * BLK, HD), jnp.float32),
            pltpu.VMEM((GRP * BLK, TOK), jnp.float32),
            pltpu.VMEM((GRP * BLK, TOK), jnp.float32),
            pltpu.VMEM((GRP * BLK, TOK), jnp.bfloat16),
            pltpu.VMEM((GRP * BLK, TOK), jnp.bfloat16),
            pltpu.VMEM((GRP * BLK, HD), jnp.float32),
            pltpu.VMEM((GRP * BLK, HD), jnp.float32),
            pltpu.SemaphoreType.DMA((len(spec),)),
        ],
        compiler_params=pltpu.CompilerParams(vmem_limit_bytes=16 << 20),
        cost_estimate=pl.CostEstimate(
            flops=(span[1] - span[0]) * 1_500_000_000,
            bytes_accessed=4_000_000,
            transcendentals=(span[1] - span[0]) * 2_000_000,
        ),
    )(doc, q, *units)


def along_z(v, step):
    pairs = [(ZN * x + z, ZN * x + (z + step) % ZN) for x in range(XN) for z in range(ZN)]
    return lax.ppermute(v, "seq", pairs)


def along_x(v, first_row):
    pairs = [(ZN * x + z, ZN * (x + 1) + z) for x in range(first_row, XN - 1) for z in range(ZN)]
    return lax.ppermute(v, "seq", pairs)


def from_corner(own):
    return lax.ppermute(own, "seq", [(ZN - 1, ZN * (XN - 1))])


def gather_apart(own, z):
    x1 = along_x(own, 0)
    below_own = along_z(own, 1)
    corner = from_corner(own)
    x2 = along_x(x1, 1)
    below_x1 = along_z(x1, 1)
    above_x1 = along_z(x1, -1)
    below_x2 = along_z(x2, 1)
    above_mixed = along_z(jnp.where(z == 0, own, x2), -1)
    far_x1 = along_z(above_x1, -1)
    far_mixed = along_z(jnp.where((z == 1) | (z == 2), below_own, below_x2), 1)
    return [
        own,
        x1,
        x2,
        below_own,
        below_x1,
        below_x2,
        above_mixed,
        above_x1,
        far_mixed,
        far_x1,
        corner,
    ]


def add_kernel(turn, ra_ref, rb_ref, p_ref, na_ref, nb_ref):
    rows, half = ra_ref.shape
    n = lax.axis_size("head")
    me = lax.axis_index("head")
    ka = pl.multiple_of((me + 2 * n - 2 - turn) % n * rows, rows)
    kb = pl.multiple_of((me + 2 + turn) % n * rows, rows)
    na_ref[...] = ra_ref[...] + p_ref[pl.ds(ka, rows), :half]
    nb_ref[...] = rb_ref[...] + p_ref[pl.ds(kb, rows), half:]


def ring_add(turn, ra, rb, partial):
    return pl.pallas_call(
        functools.partial(add_kernel, turn),
        name="ring_add",
        out_shape=[jax.ShapeDtypeStruct(ra.shape, ra.dtype)] * 2,
        in_specs=[pl.BlockSpec(memory_space=pltpu.VMEM)] * 3,
        out_specs=[pl.BlockSpec(memory_space=pltpu.VMEM)] * 2,
        compiler_params=pltpu.CompilerParams(vmem_limit_bytes=16 << 20),
        cost_estimate=pl.CostEstimate(
            flops=100_000_000, bytes_accessed=12 * ra.size, transcendentals=0
        ),
    )(ra, rb, partial)


def around(v, step):
    n = lax.axis_size("head")
    return lax.ppermute(v, "head", [(i, (i + step) % n) for i in range(n)])


def first_blocks(partial):
    me = lax.axis_index("head")
    n = lax.axis_size("head")
    rows = partial.shape[0] // n
    half = partial.shape[1] // 2
    a = lax.dynamic_slice(partial, ((me + n - 1) % n * rows, 0), (rows, half))
    b = lax.dynamic_slice(partial, ((me + 1) % n * rows, half), (rows, half))
    return a, b


def ring_step(turn, a, b, partial):
    a = around(a, 1)
    b = around(b, -1)
    return ring_add(turn, a, b, partial)


def swapped(v):
    return lax.ppermute(v, "batch", [(0, 1), (1, 0)])


def on_device(queries, key_states, value_vectors, block_doc, out_weight):
    core = lax.axis_index("batch")
    first = core == 0
    q2 = queries[0].reshape(TOK, 2 * GRP * HD)
    halves_q = (q2[:, : GRP * HD], q2[:, GRP * HD :])
    halves_kv = tuple(
        jnp.stack([key_states[0, :, h], value_vectors[0, :, h]], axis=0) for h in range(2)
    )
    kv_mine = jnp.where(first, halves_kv[0], halves_kv[1])
    kv_theirs = swapped(jnp.where(first, halves_kv[1], halves_kv[0]))
    q_mine = jnp.where(first, halves_q[0], halves_q[1])
    q_theirs = swapped(jnp.where(first, halves_q[1], halves_q[0]))
    doc_theirs = swapped(block_doc)

    def of(sequence, mine, theirs):
        return jnp.where(core == sequence, mine, theirs)

    def project(attended):
        other = swapped(attended)
        both = jnp.where(
            first,
            jnp.concatenate([attended, other], axis=1),
            jnp.concatenate([other, attended], axis=1),
        )
        return jnp.dot(both, out_weight, preferred_element_type=jnp.float32).astype(jnp.bfloat16)

    tie = lax.optimization_barrier
    z = lax.axis_index("seq") % ZN
    units0 = gather_apart(of(0, kv_mine, kv_theirs), z)

    own1, units0[2] = tie((of(1, kv_mine, kv_theirs), units0[2]))
    y1 = along_x(own1, 0)
    y2 = along_x(y1, 1)
    stack1 = jnp.stack([own1, y1, y2])
    up1 = jnp.stack([jnp.where(z == 0, own1, y2), y1])
    units0, stack1, up1 = tie((units0, stack1, up1))
    below1 = along_z(stack1, 1)
    above1 = along_z(up1, -1)
    corner1 = from_corner(own1)
    attended0 = attention(
        of(0, block_doc, doc_theirs), of(0, q_mine, q_theirs), units0, APART, (0, BPD)
    )
    partial0 = project(attended0)
    a0, b0 = first_blocks(partial0)

    (below1, above1), _ = tie(((below1, above1), (a0, b0)))
    far_mixed1 = along_z(jnp.where((z == 1) | (z == 2), below1[0], below1[2]), 1)
    far_x1 = along_z(above1[1], -1)
    units1 = [stack1, below1, above1, far_mixed1, far_x1, corner1]
    doc1, q1 = of(1, block_doc, doc_theirs), of(1, q_mine, q_theirs)
    a0, b0 = ring_step(0, a0, b0, partial0)
    upper = attention(doc1, q1, units1, STACKED, (0, BPD // 2))
    a0, b0 = ring_step(1, a0, b0, partial0)
    lower = attention(doc1, q1, units1, STACKED, (BPD // 2, BPD))
    a0, b0 = ring_step(2, a0, b0, partial0)
    partial1 = project(jnp.concatenate([upper, lower], axis=0))
    a1, b1 = first_blocks(partial1)
    for turn in range(3):
        a1, b1 = ring_step(turn, a1, b1, partial1)
    sum0 = jnp.concatenate([a0, b0], axis=1)
    sum1 = jnp.concatenate([a1, b1], axis=1)
    return jnp.stack([sum0, sum1], axis=1)


def solution(mesh):
    return jax.shard_map(
        on_device,
        mesh=mesh,
        in_specs=(
            P("batch", "seq", "head", None),
            P("batch", "seq", "head", None),
            P("batch", "seq", "head", None),
            P("batch", None),
            P("head", "batch"),
        ),
        out_specs=P(("seq", "head"), None, "batch"),
        check_vma=False,
    )
```

```python
import functools
import math

import jax
import jax.numpy as jnp
from jax import lax
from jax.experimental import pallas as pl
from jax.experimental.pallas import tpu as pltpu
from jax.sharding import PartitionSpec as P


XN = 4
ZN = 4
TOK = 512
BLK = 128
HD = 128
GRP = 4
BPD = TOK // BLK
REACH = 9
SLOTS = REACH + 1
STREAMS = 2
SCALE = math.log2(math.e) / math.sqrt(HD)
NEG = -1e30


NAMES = (
    "own",
    "x1",
    "x2",
    "below_own",
    "below_x1",
    "below_x2",
    "above_mixed",
    "above_x1",
    "far_mixed",
    "far_x1",
    "corner",
)


def unit_source(name, x, z):
    below, above, far = (z + ZN - 1) % ZN, (z + 1) % ZN, (z + 2) % ZN
    at = {
        "own": (x, z),
        "x1": (x - 1, z),
        "x2": (x - 2, z),
        "below_own": (x, below),
        "below_x1": (x - 1, below),
        "below_x2": (x - 2, below),
        "above_mixed": (jnp.where(z == ZN - 1, x, x - 2), above),
        "above_x1": (x - 1, above),
        "far_mixed": (jnp.where(z >= 2, x, x - 2), far),
        "far_x1": (x - 1, far),
        "corner": (jnp.where(z == 0, x - 3, -1), ZN - 1),
    }[name]
    return ZN * at[0] + at[1]


APART = tuple((i, None) for i in range(len(NAMES)))
STACKED = (
    (0, 0),
    (0, 1),
    (0, 2),
    (1, 0),
    (1, 1),
    (1, 2),
    (2, 0),
    (2, 1),
    (3, None),
    (4, None),
    (5, None),
)


def attn_kernel(spec, n, span, doc_ref, q_ref, *refs):
    unit_refs = refs[:n]
    o_ref = refs[n]
    kv, qs, m_ref, l_ref, acc_ref, s_a, s_b, p_a, p_b, a_a, a_b, sems = refs[n + 1 :]
    s_idx = lax.axis_index("seq")
    x_idx = s_idx // ZN
    z_idx = s_idx % ZN
    first_doc = doc_ref[0, BPD * s_idx]

    copies = []
    for i, (operand, at) in enumerate(spec):
        src = unit_source(NAMES[i], x_idx, z_idx)
        delta = s_idx - src
        safe = jnp.maximum(src, 0)
        need = (
            (src >= 0)
            & (delta >= 0)
            & (delta <= REACH)
            & (doc_ref[0, BPD * safe + BPD - 1] >= first_doc)
        )
        slot = jnp.clip(delta, 0, REACH)
        unit = unit_refs[operand]
        if at is not None:
            unit = unit.at[at]
        copy = pltpu.make_async_copy(unit, kv.at[slot], sems.at[i])
        copies.append((need, copy))
    for need, copy in copies:
        pl.when(need)(copy.start)
    for need, copy in copies:
        pl.when(need)(copy.wait)

    def score(dst, slot, mask=None):
        s = lax.dot_general(
            qs[...], kv[slot, 0], (((1,), (1,)), ((), ())), preferred_element_type=jnp.float32
        )
        if mask is None:
            dst[...] = s
        else:
            for h in range(GRP):
                rows = slice(h * BLK, (h + 1) * BLK)
                dst[rows] = jnp.where(mask, s[rows], NEG)

    def soften(src, p_dst, a_dst):
        for h in range(GRP):
            rows = slice(h * BLK, (h + 1) * BLK)
            sh = src[rows]
            m_prev = m_ref[rows]
            m_new = jnp.maximum(m_prev, jnp.max(sh, axis=1, keepdims=True))
            m_wide = jnp.concatenate([m_new] * (TOK // HD), axis=1)
            p = jnp.exp2((sh - m_wide) * SCALE)
            alpha = jnp.exp2((m_prev - m_new) * SCALE)
            part_sum = p[:, 0:HD]
            for c in range(1, TOK // HD):
                part_sum = part_sum + p[:, c * HD : (c + 1) * HD]
            l_ref[rows] = l_ref[rows] * alpha + part_sum
            m_ref[rows] = m_new
            a_dst[rows] = alpha
            p_dst[rows] = p.astype(jnp.bfloat16)

    def mix(p_src, a_src, slot):
        pv = jnp.dot(p_src[...], kv[slot, 1], preferred_element_type=jnp.float32)
        acc_ref[...] = acc_ref[...] * a_src[...] + pv

    @pl.loop(span[0], span[1])
    def _(j):
        for h in range(GRP):
            qs[h * BLK : (h + 1) * BLK] = q_ref[
                pl.ds(pl.multiple_of(j * BLK, BLK), BLK), h * HD : (h + 1) * HD
            ]
        m_ref[...] = jnp.full_like(m_ref, NEG)
        l_ref[...] = jnp.zeros_like(l_ref)
        acc_ref[...] = jnp.zeros_like(acc_ref)
        doc_q = doc_ref[0, BPD * s_idx + j]
        full = jnp.int32(0)
        some = jnp.int32(0)
        for d in range(1, REACH + 1):
            src = s_idx - d
            safe = jnp.maximum(src, 0)
            valid = src >= 0
            full = full + (valid & (doc_ref[0, BPD * safe] == doc_q)).astype(jnp.int32)
            some = some + (valid & (doc_ref[0, BPD * safe + BPD - 1] == doc_q)).astype(jnp.int32)
        key_pos = lax.broadcasted_iota(jnp.int32, (BLK, TOK), 1)
        row_pos = lax.broadcasted_iota(jnp.int32, (BLK, TOK), 0) + j * BLK

        def hidden_keys(unit):
            hidden = jnp.int32(0)
            for b in range(BPD - 1):
                hidden = hidden + (doc_ref[0, BPD * unit + b] < doc_q).astype(jnp.int32)
            return hidden * BLK

        score(s_b, 0, (key_pos <= row_pos) & (key_pos >= hidden_keys(s_idx)))
        soften(s_b, p_b, a_b)

        edge = jnp.minimum(full + 1, REACH)

        @pl.when(some > full)
        def _():
            score(s_a, edge, key_pos >= hidden_keys(jnp.maximum(s_idx - edge, 0)))
            mix(p_b, a_b, 0)
            soften(s_a, p_b, a_b)

        pend = jnp.where(some > full, edge, 0)
        odd = full % 2

        @pl.when(odd == 1)
        def _():
            score(s_a, 1)
            mix(p_b, a_b, pend)
            soften(s_a, p_b, a_b)

        pend = jnp.where(odd == 1, 1, pend)

        @pl.when(full > 1)
        def _():
            score(s_a, 1 + odd)

        @pl.loop(0, full // 2)
        def _(i):
            t = 1 + odd + 2 * i
            score(s_b, t + 1)
            soften(s_a, p_a, a_a)
            mix(p_b, a_b, jnp.where(i == 0, pend, t - 1))
            score(s_a, jnp.minimum(t + 2, full))
            soften(s_b, p_b, a_b)
            mix(p_a, a_a, t)

        mix(p_b, a_b, jnp.where(full > 1, full, pend))

        for h in range(GRP):
            rows = slice(h * BLK, (h + 1) * BLK)
            total = jnp.sum(l_ref[rows], axis=1, keepdims=True)
            o_ref[pl.ds(pl.multiple_of((j - span[0]) * BLK, BLK), BLK), h * HD : (h + 1) * HD] = (
                acc_ref[rows] / total
            ).astype(o_ref.dtype)


def attention(doc, q, units, spec, span):
    n = len(units)
    return pl.pallas_call(
        functools.partial(attn_kernel, spec, n, span),
        name="attend",
        out_shape=jax.ShapeDtypeStruct(((span[1] - span[0]) * BLK, GRP * HD), jnp.bfloat16),
        in_specs=[
            pl.BlockSpec(memory_space=pltpu.SMEM),
            pl.BlockSpec(memory_space=pltpu.VMEM),
        ]
        + [pl.BlockSpec(memory_space=pl.ANY)] * n,
        out_specs=pl.BlockSpec(memory_space=pltpu.VMEM),
        scratch_shapes=[
            pltpu.VMEM((SLOTS, 2, TOK, HD), jnp.bfloat16),
            pltpu.VMEM((GRP * BLK, HD), jnp.bfloat16),
            pltpu.VMEM((GRP * BLK, HD), jnp.float32),
            pltpu.VMEM((GRP * BLK, HD), jnp.float32),
            pltpu.VMEM((GRP * BLK, HD), jnp.float32),
            pltpu.VMEM((GRP * BLK, TOK), jnp.float32),
            pltpu.VMEM((GRP * BLK, TOK), jnp.float32),
            pltpu.VMEM((GRP * BLK, TOK), jnp.bfloat16),
            pltpu.VMEM((GRP * BLK, TOK), jnp.bfloat16),
            pltpu.VMEM((GRP * BLK, HD), jnp.float32),
            pltpu.VMEM((GRP * BLK, HD), jnp.float32),
            pltpu.SemaphoreType.DMA((len(spec),)),
        ],
        compiler_params=pltpu.CompilerParams(vmem_limit_bytes=16 << 20),
        cost_estimate=pl.CostEstimate(
            flops=(span[1] - span[0]) * 1_500_000_000,
            bytes_accessed=4_000_000,
            transcendentals=(span[1] - span[0]) * 2_000_000,
        ),
    )(doc, q, *units)


def along_z(v, step):
    pairs = [(ZN * x + z, ZN * x + (z + step) % ZN) for x in range(XN) for z in range(ZN)]
    return lax.ppermute(v, "seq", pairs)


def along_x(v, step):
    pairs = [(ZN * x + z, ZN * (x + step) + z) for x in range(XN - step) for z in range(ZN)]
    return lax.ppermute(v, "seq", pairs)


def from_corner(own):
    return lax.ppermute(own, "seq", [(ZN - 1, ZN * (XN - 1))])


def gather_apart(own, z):
    x1 = along_x(own, 1)
    x2 = along_x(own, 2)
    below_own = along_z(own, 1)
    corner = from_corner(own)
    below_x1 = along_z(x1, 1)
    above_x1 = along_z(x1, -1)
    below_x2 = along_z(x2, 1)
    above_mixed = along_z(jnp.where(z == 0, own, x2), -1)
    far_x1 = along_z(above_x1, -1)
    far_mixed = along_z(jnp.where((z == 1) | (z == 2), below_own, below_x2), 1)
    return [
        own,
        x1,
        x2,
        below_own,
        below_x1,
        below_x2,
        above_mixed,
        above_x1,
        far_mixed,
        far_x1,
        corner,
    ]


def add_kernel(turn, first_col, ra_ref, rb_ref, p_ref, na_ref, nb_ref):
    rows, width = ra_ref.shape
    n = lax.axis_size("head")
    me = lax.axis_index("head")
    half = p_ref.shape[1] // 2
    ka = pl.multiple_of((me + 2 * n - 2 - turn) % n * rows, rows)
    kb = pl.multiple_of((me + 2 + turn) % n * rows, rows)
    c = first_col
    na_ref[...] = ra_ref[...] + p_ref[pl.ds(ka, rows), c : c + width]
    nb_ref[...] = rb_ref[...] + p_ref[pl.ds(kb, rows), half + c : half + c + width]


def ring_add(turn, first_col, ra, rb, partial):
    return pl.pallas_call(
        functools.partial(add_kernel, turn, first_col),
        name="ring_add",
        out_shape=[jax.ShapeDtypeStruct(ra.shape, ra.dtype)] * 2,
        in_specs=[pl.BlockSpec(memory_space=pltpu.VMEM)] * 3,
        out_specs=[pl.BlockSpec(memory_space=pltpu.VMEM)] * 2,
        compiler_params=pltpu.CompilerParams(vmem_limit_bytes=16 << 20),
        cost_estimate=pl.CostEstimate(
            flops=100_000_000, bytes_accessed=12 * ra.size, transcendentals=0
        ),
    )(ra, rb, partial)


def around(v, step):
    n = lax.axis_size("head")
    return lax.ppermute(v, "head", [(i, (i + step) % n) for i in range(n)])


def first_kernel(own_ref, other_ref, w_ref, a_ref, b_ref):
    n = lax.axis_size("head")
    me = lax.axis_index("head")
    core = lax.axis_index("batch")
    depth = own_ref.shape[1]
    rows, half = a_ref.shape
    mine = pl.ds(pl.multiple_of(core * depth, depth), depth)
    theirs = pl.ds(pl.multiple_of((1 - core) * depth, depth), depth)
    tile = 512
    for out_ref, block, base in ((a_ref, (me + n - 1) % n, 0), (b_ref, (me + 1) % n, half)):
        at = pl.ds(pl.multiple_of(block * rows, rows), rows)
        own, other = own_ref[at], other_ref[at]

        @pl.loop(0, half // tile)
        def _(i):
            start = pl.multiple_of(i * tile, tile)
            cols = pl.ds(pl.multiple_of(base + i * tile, tile), tile)
            out_ref[:, pl.ds(start, tile)] = (
                jnp.dot(own, w_ref[mine, cols], preferred_element_type=jnp.float32)
                + jnp.dot(other, w_ref[theirs, cols], preferred_element_type=jnp.float32)
            ).astype(out_ref.dtype)


def first_blocks(own, other, weight):
    rows = own.shape[0] // lax.axis_size("head")
    half = weight.shape[1] // 2
    return pl.pallas_call(
        first_kernel,
        name="first_blocks",
        out_shape=[jax.ShapeDtypeStruct((rows, half), jnp.bfloat16)] * 2,
        in_specs=[pl.BlockSpec(memory_space=pltpu.VMEM)] * 3,
        out_specs=[pl.BlockSpec(memory_space=pltpu.VMEM)] * 2,
        compiler_params=pltpu.CompilerParams(vmem_limit_bytes=24 << 20),
        cost_estimate=pl.CostEstimate(
            flops=4 * rows * half * weight.shape[0], bytes_accessed=12 << 20, transcendentals=0
        ),
    )(own, other, weight)


def ring_step(turn, a, b, partial, first_col=0):
    a = around(a, 1)
    b = around(b, -1)
    return ring_add(turn, first_col, a, b, partial)


def swapped(v):
    return lax.ppermute(v, "batch", [(0, 1), (1, 0)])


def on_device(queries, key_states, value_vectors, block_doc, out_weight):
    core = lax.axis_index("batch")
    first = core == 0
    q2 = queries[0].reshape(TOK, 2 * GRP * HD)
    halves_q = (q2[:, : GRP * HD], q2[:, GRP * HD :])
    halves_kv = tuple(
        jnp.stack([key_states[0, :, h], value_vectors[0, :, h]], axis=0) for h in range(2)
    )
    kv_mine = jnp.where(first, halves_kv[0], halves_kv[1])
    kv_theirs = swapped(jnp.where(first, halves_kv[1], halves_kv[0]))
    q_mine = jnp.where(first, halves_q[0], halves_q[1])
    q_theirs = swapped(jnp.where(first, halves_q[1], halves_q[0]))
    doc_theirs = swapped(block_doc)

    def of(sequence, mine, theirs):
        return jnp.where(core == sequence, mine, theirs)

    def project(attended, other):
        both = jnp.where(
            first,
            jnp.concatenate([attended, other], axis=1),
            jnp.concatenate([other, attended], axis=1),
        )
        return jnp.dot(both, out_weight, preferred_element_type=jnp.float32).astype(jnp.bfloat16)

    tie = lax.optimization_barrier
    z = lax.axis_index("seq") % ZN
    units0 = gather_apart(of(0, kv_mine, kv_theirs), z)

    own1 = of(1, kv_mine, kv_theirs)
    y1 = along_x(own1, 1)
    y2 = along_x(own1, 2)
    corner1 = from_corner(own1)
    units0, (own1, y1, y2) = tie((units0, (own1, y1, y2)))
    stack1 = jnp.stack([own1, y1, y2])
    up1 = jnp.stack([jnp.where(z == 0, own1, y2), y1])
    below1 = along_z(stack1, 1)
    above1 = along_z(up1, -1)
    attended0 = attention(
        of(0, block_doc, doc_theirs), of(0, q_mine, q_theirs), units0, APART, (0, BPD)
    )
    other0 = swapped(attended0)
    a0, b0 = first_blocks(attended0, other0, out_weight)
    _, (attended0, other0) = tie(((a0, b0), (attended0, other0)))
    partial0 = project(attended0, other0)

    (below1, above1), _ = tie(((below1, above1), (a0, b0)))
    far_mixed1 = along_z(jnp.where((z == 1) | (z == 2), below1[0], below1[2]), 1)
    far_x1 = along_z(above1[1], -1)
    units1 = [stack1, below1, above1, far_mixed1, far_x1, corner1]
    doc1, q1 = of(1, block_doc, doc_theirs), of(1, q_mine, q_theirs)
    a0, b0 = ring_step(0, a0, b0, partial0)
    upper = attention(doc1, q1, units1, STACKED, (0, BPD // 2))
    a0, b0 = ring_step(1, a0, b0, partial0)
    lower = attention(doc1, q1, units1, STACKED, (BPD // 2, BPD))
    a0, b0 = ring_step(2, a0, b0, partial0)
    attended1 = jnp.concatenate([upper, lower], axis=0)
    other1 = swapped(attended1)
    a1, b1 = first_blocks(attended1, other1, out_weight)
    _, (attended1, other1) = tie(((a1, b1), (attended1, other1)))
    partial1 = project(attended1, other1)
    width = a1.shape[1] // STREAMS
    tails = []
    for i in range(STREAMS):
        cols = slice(i * width, (i + 1) * width)
        a, b = a1[:, cols], b1[:, cols]
        for turn in range(3):
            a, b = ring_step(turn, a, b, partial1, i * width)
        tails.append((a, b))
    sum0 = jnp.concatenate([a0, b0], axis=1)
    sum1 = jnp.concatenate([t[0] for t in tails] + [t[1] for t in tails], axis=1)
    spot = lax.broadcasted_iota(jnp.int32, (1, 2, 1), 1)
    return jnp.where(spot == 0, sum0[:, None], sum1[:, None])


def solution(mesh):
    return jax.shard_map(
        on_device,
        mesh=mesh,
        in_specs=(
            P("batch", "seq", "head", None),
            P("batch", "seq", "head", None),
            P("batch", "seq", "head", None),
            P("batch", None),
            P("head", "batch"),
        ),
        out_specs=P(("seq", "head"), None, "batch"),
        check_vma=False,
    )
```

```python
import functools
import math

import jax
import jax.numpy as jnp
from jax import lax
from jax.experimental import pallas as pl
from jax.experimental.pallas import tpu as pltpu
from jax.sharding import PartitionSpec as P


XN = 4
ZN = 4
TOK = 512
BLK = 128
HD = 128
GRP = 4
BPD = TOK // BLK
REACH = 9
SLOTS = REACH + 1
STREAMS = 2
SCALE = math.log2(math.e) / math.sqrt(HD)
NEG = -1e30


NAMES = (
    "own",
    "x1",
    "x2",
    "below_own",
    "below_x1",
    "below_x2",
    "above_mixed",
    "above_x1",
    "far_mixed",
    "far_x1",
    "corner",
)


def unit_source(name, x, z):
    below, above, far = (z + ZN - 1) % ZN, (z + 1) % ZN, (z + 2) % ZN
    at = {
        "own": (x, z),
        "x1": (x - 1, z),
        "x2": (x - 2, z),
        "below_own": (x, below),
        "below_x1": (x - 1, below),
        "below_x2": (x - 2, below),
        "above_mixed": (jnp.where(z == ZN - 1, x, x - 2), above),
        "above_x1": (x - 1, above),
        "far_mixed": (jnp.where(z >= 2, x, x - 2), far),
        "far_x1": (x - 1, far),
        "corner": (jnp.where(z == 0, x - 3, -1), ZN - 1),
    }[name]
    return ZN * at[0] + at[1]


APART = tuple((i, None) for i in range(len(NAMES)))
STACKED = (
    (0, 0),
    (0, 1),
    (0, 2),
    (1, 0),
    (1, 1),
    (1, 2),
    (2, 0),
    (2, 1),
    (3, None),
    (4, None),
    (5, None),
)


def turn_block(pair, step, head):
    if pair == 0:
        return (head + BPD - 1 + 2 * step) % BPD
    return (head + BPD // 2 * (1 - step)) % BPD


def attn_kernel(spec, n, pair, doc_ref, q_ref, *refs):
    unit_refs = refs[:n]
    o_ref = refs[n]
    kv, qs, m_ref, l_ref, acc_ref, s_a, s_b, p_a, p_b, a_a, a_b, sems = refs[n + 1 :]
    s_idx = lax.axis_index("seq")
    x_idx = s_idx // ZN
    z_idx = s_idx % ZN
    first_doc = doc_ref[0, BPD * s_idx]

    copies = []
    for i, (operand, at) in enumerate(spec):
        src = unit_source(NAMES[i], x_idx, z_idx)
        delta = s_idx - src
        safe = jnp.maximum(src, 0)
        need = (
            (src >= 0)
            & (delta >= 0)
            & (delta <= REACH)
            & (doc_ref[0, BPD * safe + BPD - 1] >= first_doc)
        )
        slot = jnp.clip(delta, 0, REACH)
        unit = unit_refs[operand]
        if at is not None:
            unit = unit.at[at]
        copy = pltpu.make_async_copy(unit, kv.at[slot], sems.at[i])
        copies.append((need, copy))
    for need, copy in copies:
        pl.when(need)(copy.start)
    for need, copy in copies:
        pl.when(need)(copy.wait)

    def score(dst, slot, mask=None):
        s = lax.dot_general(
            qs[...], kv[slot, 0], (((1,), (1,)), ((), ())), preferred_element_type=jnp.float32
        )
        if mask is None:
            dst[...] = s
        else:
            for h in range(GRP):
                rows = slice(h * BLK, (h + 1) * BLK)
                dst[rows] = jnp.where(mask, s[rows], NEG)

    def soften(src, p_dst, a_dst):
        for h in range(GRP):
            rows = slice(h * BLK, (h + 1) * BLK)
            sh = src[rows]
            m_prev = m_ref[rows]
            m_new = jnp.maximum(m_prev, jnp.max(sh, axis=1, keepdims=True))
            m_wide = jnp.concatenate([m_new] * (TOK // HD), axis=1)
            p = jnp.exp2((sh - m_wide) * SCALE)
            alpha = jnp.exp2((m_prev - m_new) * SCALE)
            part_sum = p[:, 0:HD]
            for c in range(1, TOK // HD):
                part_sum = part_sum + p[:, c * HD : (c + 1) * HD]
            l_ref[rows] = l_ref[rows] * alpha + part_sum
            m_ref[rows] = m_new
            a_dst[rows] = alpha
            p_dst[rows] = p.astype(jnp.bfloat16)

    def mix(p_src, a_src, slot):
        pv = jnp.dot(p_src[...], kv[slot, 1], preferred_element_type=jnp.float32)
        acc_ref[...] = acc_ref[...] * a_src[...] + pv

    head = lax.axis_index("head")

    @pl.loop(0, 2)
    def _(step):
        j = turn_block(pair, step, head)
        for h in range(GRP):
            qs[h * BLK : (h + 1) * BLK] = q_ref[
                pl.ds(pl.multiple_of(j * BLK, BLK), BLK), h * HD : (h + 1) * HD
            ]
        m_ref[...] = jnp.full_like(m_ref, NEG)
        l_ref[...] = jnp.zeros_like(l_ref)
        acc_ref[...] = jnp.zeros_like(acc_ref)
        doc_q = doc_ref[0, BPD * s_idx + j]
        full = jnp.int32(0)
        some = jnp.int32(0)
        for d in range(1, REACH + 1):
            src = s_idx - d
            safe = jnp.maximum(src, 0)
            valid = src >= 0
            full = full + (valid & (doc_ref[0, BPD * safe] == doc_q)).astype(jnp.int32)
            some = some + (valid & (doc_ref[0, BPD * safe + BPD - 1] == doc_q)).astype(jnp.int32)
        key_pos = lax.broadcasted_iota(jnp.int32, (BLK, TOK), 1)
        row_pos = lax.broadcasted_iota(jnp.int32, (BLK, TOK), 0) + j * BLK

        def hidden_keys(unit):
            hidden = jnp.int32(0)
            for b in range(BPD - 1):
                hidden = hidden + (doc_ref[0, BPD * unit + b] < doc_q).astype(jnp.int32)
            return hidden * BLK

        edge = jnp.minimum(full + 1, REACH)
        odd = full % 2
        has_edge = (some > full).astype(jnp.int32)

        def single_slot(k):
            return jnp.where(k == 0, 0, jnp.where((k == 1) & (has_edge == 1), edge, 1))

        singles = 1 + has_edge + odd

        @pl.loop(0, singles)
        def _(k):
            slot = single_slot(k)
            low = hidden_keys(jnp.maximum(s_idx - slot, 0))
            high = jnp.where(k == 0, 0, TOK)
            score(s_a, slot, (key_pos <= row_pos + high) & (key_pos >= low))

            @pl.when(k > 0)
            def _():
                mix(p_b, a_b, single_slot(k - 1))

            soften(s_a, p_b, a_b)

        pend = single_slot(singles - 1)

        @pl.when(full > 1)
        def _():
            score(s_a, 1 + odd)

        @pl.loop(0, full // 2)
        def _(i):
            t = 1 + odd + 2 * i
            score(s_b, t + 1)
            soften(s_a, p_a, a_a)
            mix(p_b, a_b, jnp.where(i == 0, pend, t - 1))
            score(s_a, jnp.minimum(t + 2, full))
            soften(s_b, p_b, a_b)
            mix(p_a, a_a, t)

        mix(p_b, a_b, jnp.where(full > 1, full, pend))

        for h in range(GRP):
            rows = slice(h * BLK, (h + 1) * BLK)
            total = jnp.sum(l_ref[rows], axis=1, keepdims=True)
            o_ref[pl.ds(pl.multiple_of(step * BLK, BLK), BLK), h * HD : (h + 1) * HD] = (
                acc_ref[rows] / total
            ).astype(o_ref.dtype)


def attention(doc, q, units, spec, pair):
    n = len(units)
    return pl.pallas_call(
        functools.partial(attn_kernel, spec, n, pair),
        name="attend",
        out_shape=jax.ShapeDtypeStruct((2 * BLK, GRP * HD), jnp.bfloat16),
        in_specs=[
            pl.BlockSpec(memory_space=pltpu.SMEM),
            pl.BlockSpec(memory_space=pltpu.VMEM),
        ]
        + [pl.BlockSpec(memory_space=pl.ANY)] * n,
        out_specs=pl.BlockSpec(memory_space=pltpu.VMEM),
        scratch_shapes=[
            pltpu.VMEM((SLOTS, 2, TOK, HD), jnp.bfloat16),
            pltpu.VMEM((GRP * BLK, HD), jnp.bfloat16),
            pltpu.VMEM((GRP * BLK, HD), jnp.float32),
            pltpu.VMEM((GRP * BLK, HD), jnp.float32),
            pltpu.VMEM((GRP * BLK, HD), jnp.float32),
            pltpu.VMEM((GRP * BLK, TOK), jnp.float32),
            pltpu.VMEM((GRP * BLK, TOK), jnp.float32),
            pltpu.VMEM((GRP * BLK, TOK), jnp.bfloat16),
            pltpu.VMEM((GRP * BLK, TOK), jnp.bfloat16),
            pltpu.VMEM((GRP * BLK, HD), jnp.float32),
            pltpu.VMEM((GRP * BLK, HD), jnp.float32),
            pltpu.SemaphoreType.DMA((len(spec),)),
        ],
        compiler_params=pltpu.CompilerParams(vmem_limit_bytes=16 << 20),
        cost_estimate=pl.CostEstimate(
            flops=3_000_000_000,
            bytes_accessed=4_000_000,
            transcendentals=4_000_000,
        ),
    )(doc, q, *units)


def along_z(v, step):
    pairs = [(ZN * x + z, ZN * x + (z + step) % ZN) for x in range(XN) for z in range(ZN)]
    return lax.ppermute(v, "seq", pairs)


def along_x(v, step):
    pairs = [(ZN * x + z, ZN * (x + step) + z) for x in range(XN - step) for z in range(ZN)]
    return lax.ppermute(v, "seq", pairs)


def up_row(v):
    pairs = [(ZN * x + z, ZN * x + z + 1) for x in range(XN) for z in range(ZN - 1)]
    pairs.append((ZN - 1, 0))
    return lax.ppermute(v, "seq", pairs)


def from_corner(v):
    return lax.ppermute(v, "seq", [(0, ZN * (XN - 1))])


def gather_apart(own, z):
    x1 = along_x(own, 1)
    x2 = along_x(own, 2)
    below_own = up_row(own)
    corner = from_corner(below_own)
    below_x1 = along_z(x1, 1)
    above_x1 = along_z(x1, -1)
    below_x2 = along_z(x2, 1)
    above_mixed = along_z(jnp.where(z == 0, own, x2), -1)
    far_x1 = along_z(above_x1, -1)
    far_mixed = along_z(jnp.where((z == 1) | (z == 2), below_own, below_x2), 1)
    return [
        own,
        x1,
        x2,
        below_own,
        below_x1,
        below_x2,
        above_mixed,
        above_x1,
        far_mixed,
        far_x1,
        corner,
    ]


TURNS = ((1, 0, 0), (0, 1, 0), (1, 1, 1))


def add_kernel(turn, first_col, last_col, ra_ref, rb_ref, p_ref, na_ref, nb_ref):
    rows = ra_ref.shape[0]
    half = p_ref.shape[1] // 2
    _, ka, kb = TURNS[turn]
    skip = ra_ref.shape[1] != last_col - first_col
    took = slice(first_col, last_col) if skip else slice(None)
    step = 32

    @pl.loop(0, rows // step)
    def _(i):
        at = pl.ds(pl.multiple_of(i * step, step), step)
        pa = pl.ds(pl.multiple_of(ka * rows + i * step, step), step)
        pb = pl.ds(pl.multiple_of(kb * rows + i * step, step), step)
        na_ref[at] = ra_ref[at, took] + p_ref[pa, first_col:last_col]
        nb_ref[at] = rb_ref[at, took] + p_ref[pb, half + first_col : half + last_col]


def ring_add(turn, first_col, last_col, ra, rb, partials):
    shape = (ra.shape[0], last_col - first_col)
    return pl.pallas_call(
        functools.partial(add_kernel, turn, first_col, last_col),
        name="ring_add",
        out_shape=[jax.ShapeDtypeStruct(shape, ra.dtype)] * 2,
        in_specs=[pl.BlockSpec(memory_space=pltpu.VMEM)] * 3,
        out_specs=[pl.BlockSpec(memory_space=pltpu.VMEM)] * 2,
        compiler_params=pltpu.CompilerParams(vmem_limit_bytes=16 << 20),
        cost_estimate=pl.CostEstimate(
            flops=100_000_000, bytes_accessed=12 * ra.size, transcendentals=0
        ),
    )(ra, rb, partials[TURNS[turn][0]])


def around(v, step):
    n = lax.axis_size("head")
    return lax.ppermute(v, "head", [(i, (i + step) % n) for i in range(n)])


def first_kernel(own_ref, other_ref, w_ref, a_ref, b_ref):
    core = lax.axis_index("batch")
    depth = own_ref.shape[1]
    rows, half = a_ref.shape
    mine = pl.ds(pl.multiple_of(core * depth, depth), depth)
    theirs = pl.ds(pl.multiple_of((1 - core) * depth, depth), depth)
    tile = 512
    for i, out_ref in enumerate((a_ref, b_ref)):
        own, other = own_ref[i * rows : (i + 1) * rows], other_ref[i * rows : (i + 1) * rows]

        @pl.loop(0, half // tile)
        def _(t):
            start = pl.multiple_of(t * tile, tile)
            cols = pl.ds(pl.multiple_of(i * half + t * tile, tile), tile)
            out_ref[:, pl.ds(start, tile)] = (
                jnp.dot(own, w_ref[mine, cols], preferred_element_type=jnp.float32)
                + jnp.dot(other, w_ref[theirs, cols], preferred_element_type=jnp.float32)
            ).astype(out_ref.dtype)


def first_blocks(own, other, weight):
    rows = own.shape[0] // 2
    half = weight.shape[1] // 2
    return pl.pallas_call(
        first_kernel,
        name="first_blocks",
        out_shape=[jax.ShapeDtypeStruct((rows, half), jnp.bfloat16)] * 2,
        in_specs=[pl.BlockSpec(memory_space=pltpu.VMEM)] * 3,
        out_specs=[pl.BlockSpec(memory_space=pltpu.VMEM)] * 2,
        compiler_params=pltpu.CompilerParams(vmem_limit_bytes=24 << 20),
        cost_estimate=pl.CostEstimate(
            flops=4 * rows * half * weight.shape[0], bytes_accessed=12 << 20, transcendentals=0
        ),
    )(own, other, weight)


def ring_step(turn, a, b, partial, first_col=0):
    a, b = ring_send(a, b)
    return ring_add(turn, first_col, first_col + a.shape[1], a, b, partial)


def ring_send(a, b):
    a = around(a, 1)
    b = around(b, -1)
    return a, b


def swapped(v):
    return lax.ppermute(v, "batch", [(0, 1), (1, 0)])


def on_device(queries, key_states, value_vectors, block_doc, out_weight):
    core = lax.axis_index("batch")
    first = core == 0
    q2 = queries[0].reshape(TOK, 2 * GRP * HD)
    halves_q = (q2[:, : GRP * HD], q2[:, GRP * HD :])
    halves_kv = tuple(
        jnp.stack([key_states[0, :, h], value_vectors[0, :, h]], axis=0) for h in range(2)
    )
    kv_mine = jnp.where(first, halves_kv[0], halves_kv[1])
    kv_theirs = swapped(jnp.where(first, halves_kv[1], halves_kv[0]))
    q_mine = jnp.where(first, halves_q[0], halves_q[1])
    q_theirs = swapped(jnp.where(first, halves_q[1], halves_q[0]))
    doc_theirs = swapped(block_doc)

    def of(sequence, mine, theirs):
        return jnp.where(core == sequence, mine, theirs)

    def project(attended, other):
        both = jnp.where(
            first,
            jnp.concatenate([attended, other], axis=1),
            jnp.concatenate([other, attended], axis=1),
        )
        return jnp.dot(both, out_weight, preferred_element_type=jnp.float32).astype(jnp.bfloat16)

    tie = lax.optimization_barrier
    z = lax.axis_index("seq") % ZN
    units0 = gather_apart(of(0, kv_mine, kv_theirs), z)

    own1 = of(1, kv_mine, kv_theirs)
    edge1 = lax.ppermute(own1, "seq", [(ZN - 1, 0)])
    corner1 = from_corner(edge1)
    y1 = along_x(own1, 1)
    y2 = along_x(own1, 2)
    units0, (own1, y1, y2) = tie((units0, (own1, y1, y2)))
    stack1 = jnp.stack([own1, y1, y2])
    up1 = jnp.stack([jnp.where(z == 0, own1, y2), y1])
    below1 = along_z(stack1, 1)
    above1 = along_z(up1, -1)
    doc0, q0 = of(0, block_doc, doc_theirs), of(0, q_mine, q_theirs)
    early0 = attention(doc0, q0, units0, APART, 0)
    early0_other = swapped(early0)
    a0, b0 = first_blocks(early0, early0_other, out_weight)
    (q0, doc0, early0, early0_other), _ = tie(((q0, doc0, early0, early0_other), (a0, b0)))
    late0 = attention(doc0, q0, units0, APART, 1)
    late0_other = swapped(late0)
    late0_sum = project(late0, late0_other)
    early0_sum = project(early0, early0_other)
    partial0 = (early0_sum, late0_sum)

    (below1, above1), _ = tie(((below1, above1), (a0, b0)))
    far_mixed1 = along_z(jnp.where((z == 1) | (z == 2), below1[0], below1[2]), 1)
    far_x1 = along_z(above1[1], -1)
    units1 = [stack1, below1, above1, far_mixed1, far_x1, corner1]
    doc1, q1 = of(1, block_doc, doc_theirs), of(1, q_mine, q_theirs)
    a0, b0 = ring_step(0, a0, b0, partial0)
    early1 = attention(doc1, q1, units1, STACKED, 0)
    early1_other = swapped(early1)
    a1, b1 = first_blocks(early1, early1_other, out_weight)
    a0, b0 = ring_step(1, a0, b0, partial0)
    late1 = attention(doc1, q1, units1, STACKED, 1)
    a0, b0 = ring_step(2, a0, b0, partial0)
    late1_other = swapped(late1)
    (early1, early1_other), _ = tie(((early1, early1_other), (a1, b1)))
    late1_sum = project(late1, late1_other)
    early1_sum = project(early1, early1_other)
    partial1 = (early1_sum, late1_sum)
    width = a1.shape[1] // STREAMS
    a1, b1 = ring_send(a1, b1)
    tails = []
    for i in range(STREAMS):
        a, b = ring_add(0, i * width, (i + 1) * width, a1, b1, partial1)
        for turn in (1, 2):
            a, b = ring_step(turn, a, b, partial1, i * width)
        tails.append((a, b))
    sum0 = jnp.concatenate([a0, b0], axis=1)
    sum1 = jnp.concatenate([t[0] for t in tails] + [t[1] for t in tails], axis=1)
    spot = lax.broadcasted_iota(jnp.int32, (1, 2, 1), 1)
    return jnp.where(spot == 0, sum0[:, None], sum1[:, None])


def solution(mesh):
    return jax.shard_map(
        on_device,
        mesh=mesh,
        in_specs=(
            P("batch", "seq", "head", None),
            P("batch", "seq", "head", None),
            P("batch", "seq", "head", None),
            P("batch", None),
            P("head", "batch"),
        ),
        out_specs=P(("seq", "head"), None, "batch"),
        check_vma=False,
    )
```

```python
import functools
import math

import jax
import jax.numpy as jnp
from jax import lax
from jax.experimental import pallas as pl
from jax.experimental.pallas import tpu as pltpu
from jax.sharding import PartitionSpec as P


XN = 4
ZN = 4
TOK = 512
BLK = 128
HD = 128
GRP = 4
BPD = TOK // BLK
REACH = 9
SLOTS = REACH + 1
STREAMS = 2
SCALE = math.log2(math.e) / math.sqrt(HD)
NEG = -1e30


NAMES = (
    "own",
    "x1",
    "x2",
    "below_own",
    "below_x1",
    "below_x2",
    "above_mixed",
    "above_x1",
    "far_mixed",
    "far_x1",
    "corner",
)


def unit_source(name, x, z):
    below, above, far = (z + ZN - 1) % ZN, (z + 1) % ZN, (z + 2) % ZN
    at = {
        "own": (x, z),
        "x1": (x - 1, z),
        "x2": (x - 2, z),
        "below_own": (x, below),
        "below_x1": (x - 1, below),
        "below_x2": (x - 2, below),
        "above_mixed": (jnp.where(z == ZN - 1, x, x - 2), above),
        "above_x1": (x - 1, above),
        "far_mixed": (jnp.where(z >= 2, x, x - 2), far),
        "far_x1": (x - 1, far),
        "corner": (jnp.where(z == 0, x - 3, -1), ZN - 1),
    }[name]
    return ZN * at[0] + at[1]


APART = tuple((i, None) for i in range(len(NAMES)))
STACKED = (
    (0, 0),
    (0, 1),
    (0, 2),
    (1, 0),
    (1, 1),
    (1, 2),
    (2, 0),
    (2, 1),
    (3, None),
    (4, None),
    (5, None),
)


def turn_block(pair, step, head):
    if pair == 0:
        return (head + BPD - 1 + 2 * step) % BPD
    return (head + BPD // 2 * (1 - step)) % BPD


def attn_kernel(spec, n, pair, doc_ref, q_ref, *refs):
    unit_refs = refs[:n]
    o_ref = refs[n]
    kv, qs, m_ref, l_ref, acc_ref, s_a, s_b, p_a, p_b, a_a, a_b, sems = refs[n + 1 :]
    s_idx = lax.axis_index("seq")
    x_idx = s_idx // ZN
    z_idx = s_idx % ZN
    first_doc = doc_ref[0, BPD * s_idx]

    copies = []
    for i, (operand, at) in enumerate(spec):
        src = unit_source(NAMES[i], x_idx, z_idx)
        delta = s_idx - src
        safe = jnp.maximum(src, 0)
        need = (
            (src >= 0)
            & (delta >= 0)
            & (delta <= REACH)
            & (doc_ref[0, BPD * safe + BPD - 1] >= first_doc)
        )
        slot = jnp.clip(delta, 0, REACH)
        unit = unit_refs[operand]
        if at is not None:
            unit = unit.at[at]
        copy = pltpu.make_async_copy(unit, kv.at[slot], sems.at[i])
        copies.append((need, copy))
    for need, copy in copies:
        pl.when(need)(copy.start)
    for need, copy in copies:
        pl.when(need)(copy.wait)

    def score(dst, slot, mask=None):
        s = lax.dot_general(
            qs[...], kv[slot, 0], (((1,), (1,)), ((), ())), preferred_element_type=jnp.float32
        )
        if mask is None:
            dst[...] = s
        else:
            for h in range(GRP):
                rows = slice(h * BLK, (h + 1) * BLK)
                dst[rows] = jnp.where(mask, s[rows], NEG)

    def soften(src, p_dst, a_dst):
        for h in range(GRP):
            rows = slice(h * BLK, (h + 1) * BLK)
            sh = src[rows]
            m_prev = m_ref[rows]
            m_new = jnp.maximum(m_prev, jnp.max(sh, axis=1, keepdims=True))
            m_wide = jnp.concatenate([m_new] * (TOK // HD), axis=1)
            p = jnp.exp2((sh - m_wide) * SCALE)
            alpha = jnp.exp2((m_prev - m_new) * SCALE)
            part_sum = p[:, 0:HD]
            for c in range(1, TOK // HD):
                part_sum = part_sum + p[:, c * HD : (c + 1) * HD]
            l_ref[rows] = l_ref[rows] * alpha + part_sum
            m_ref[rows] = m_new
            a_dst[rows] = alpha
            p_dst[rows] = p.astype(jnp.bfloat16)

    def mix(p_src, a_src, slot):
        pv = jnp.dot(p_src[...], kv[slot, 1], preferred_element_type=jnp.float32)
        acc_ref[...] = acc_ref[...] * a_src[...] + pv

    head = lax.axis_index("head")

    @pl.loop(0, 2)
    def _(step):
        j = turn_block(pair, step, head)
        for h in range(GRP):
            qs[h * BLK : (h + 1) * BLK] = q_ref[
                pl.ds(pl.multiple_of(j * BLK, BLK), BLK), h * HD : (h + 1) * HD
            ]
        m_ref[...] = jnp.full_like(m_ref, NEG)
        l_ref[...] = jnp.zeros_like(l_ref)
        acc_ref[...] = jnp.zeros_like(acc_ref)
        doc_q = doc_ref[0, BPD * s_idx + j]
        full = jnp.int32(0)
        some = jnp.int32(0)
        for d in range(1, REACH + 1):
            src = s_idx - d
            safe = jnp.maximum(src, 0)
            valid = src >= 0
            full = full + (valid & (doc_ref[0, BPD * safe] == doc_q)).astype(jnp.int32)
            some = some + (valid & (doc_ref[0, BPD * safe + BPD - 1] == doc_q)).astype(jnp.int32)
        key_pos = lax.broadcasted_iota(jnp.int32, (BLK, TOK), 1)
        row_pos = lax.broadcasted_iota(jnp.int32, (BLK, TOK), 0) + j * BLK

        def hidden_keys(unit):
            hidden = jnp.int32(0)
            for b in range(BPD - 1):
                hidden = hidden + (doc_ref[0, BPD * unit + b] < doc_q).astype(jnp.int32)
            return hidden * BLK

        edge = jnp.minimum(full + 1, REACH)
        odd = full % 2
        has_edge = (some > full).astype(jnp.int32)

        def single_slot(k):
            return jnp.where(k == 0, 0, jnp.where((k == 1) & (has_edge == 1), edge, 1))

        singles = 1 + has_edge + odd

        @pl.loop(0, singles)
        def _(k):
            slot = single_slot(k)
            low = hidden_keys(jnp.maximum(s_idx - slot, 0))
            high = jnp.where(k == 0, 0, TOK)
            score(s_a, slot, (key_pos <= row_pos + high) & (key_pos >= low))

            @pl.when(k > 0)
            def _():
                mix(p_b, a_b, single_slot(k - 1))

            soften(s_a, p_b, a_b)

        pend = single_slot(singles - 1)

        @pl.when(full > 1)
        def _():
            score(s_a, 1 + odd)

        @pl.loop(0, full // 2)
        def _(i):
            t = 1 + odd + 2 * i
            score(s_b, t + 1)
            soften(s_a, p_a, a_a)
            mix(p_b, a_b, jnp.where(i == 0, pend, t - 1))
            score(s_a, jnp.minimum(t + 2, full))
            soften(s_b, p_b, a_b)
            mix(p_a, a_a, t)

        mix(p_b, a_b, jnp.where(full > 1, full, pend))

        for h in range(GRP):
            rows = slice(h * BLK, (h + 1) * BLK)
            total = jnp.sum(l_ref[rows], axis=1, keepdims=True)
            o_ref[pl.ds(pl.multiple_of(step * BLK, BLK), BLK), h * HD : (h + 1) * HD] = (
                acc_ref[rows] / total
            ).astype(o_ref.dtype)


def attention(doc, q, units, spec, pair):
    n = len(units)
    return pl.pallas_call(
        functools.partial(attn_kernel, spec, n, pair),
        name="attend",
        out_shape=jax.ShapeDtypeStruct((2 * BLK, GRP * HD), jnp.bfloat16),
        in_specs=[
            pl.BlockSpec(memory_space=pltpu.SMEM),
            pl.BlockSpec(memory_space=pltpu.VMEM),
        ]
        + [pl.BlockSpec(memory_space=pl.ANY)] * n,
        out_specs=pl.BlockSpec(memory_space=pltpu.VMEM),
        scratch_shapes=[
            pltpu.VMEM((SLOTS, 2, TOK, HD), jnp.bfloat16),
            pltpu.VMEM((GRP * BLK, HD), jnp.bfloat16),
            pltpu.VMEM((GRP * BLK, HD), jnp.float32),
            pltpu.VMEM((GRP * BLK, HD), jnp.float32),
            pltpu.VMEM((GRP * BLK, HD), jnp.float32),
            pltpu.VMEM((GRP * BLK, TOK), jnp.float32),
            pltpu.VMEM((GRP * BLK, TOK), jnp.float32),
            pltpu.VMEM((GRP * BLK, TOK), jnp.bfloat16),
            pltpu.VMEM((GRP * BLK, TOK), jnp.bfloat16),
            pltpu.VMEM((GRP * BLK, HD), jnp.float32),
            pltpu.VMEM((GRP * BLK, HD), jnp.float32),
            pltpu.SemaphoreType.DMA((len(spec),)),
        ],
        compiler_params=pltpu.CompilerParams(vmem_limit_bytes=16 << 20),
        cost_estimate=pl.CostEstimate(
            flops=3_000_000_000,
            bytes_accessed=4_000_000,
            transcendentals=4_000_000,
        ),
    )(doc, q, *units)


def along_z(v, step):
    pairs = [(ZN * x + z, ZN * x + (z + step) % ZN) for x in range(XN) for z in range(ZN)]
    return lax.ppermute(v, "seq", pairs)


def along_x(v, step):
    pairs = [(ZN * x + z, ZN * ((x + step) % XN) + z) for x in range(XN) for z in range(ZN)]
    return lax.ppermute(v, "seq", pairs)


def up_row(v):
    pairs = [(ZN * x + z, ZN * x + z + 1) for x in range(XN) for z in range(ZN - 1)]
    pairs.append((ZN - 1, 0))
    return lax.ppermute(v, "seq", pairs)


def from_corner(v):
    return lax.ppermute(v, "seq", [(0, ZN * (XN - 1))])


def gather_apart(own, z):
    x1 = along_x(own, 1)
    x2 = along_x(own, 2)
    below_own = up_row(own)
    corner = from_corner(below_own)
    below_x1 = along_z(x1, 1)
    above_x1 = along_z(x1, -1)
    below_x2 = along_z(x2, 1)
    above_mixed = along_z(jnp.where(z == 0, own, x2), -1)
    far_x1 = along_z(above_x1, -1)
    far_mixed = along_z(jnp.where((z == 1) | (z == 2), below_own, below_x2), 1)
    return [
        own,
        x1,
        x2,
        below_own,
        below_x1,
        below_x2,
        above_mixed,
        above_x1,
        far_mixed,
        far_x1,
        corner,
    ]


TURNS = ((1, 0, 0), (0, 1, 0), (1, 1, 1))


def add_kernel(turn, first_col, last_col, ra_ref, rb_ref, p_ref, na_ref, nb_ref):
    rows = ra_ref.shape[0]
    half = p_ref.shape[1] // 2
    _, ka, kb = TURNS[turn]
    skip = ra_ref.shape[1] != last_col - first_col
    took = slice(first_col, last_col) if skip else slice(None)
    step = 32

    @pl.loop(0, rows // step)
    def _(i):
        at = pl.ds(pl.multiple_of(i * step, step), step)
        pa = pl.ds(pl.multiple_of(ka * rows + i * step, step), step)
        pb = pl.ds(pl.multiple_of(kb * rows + i * step, step), step)
        na_ref[at] = ra_ref[at, took] + p_ref[pa, first_col:last_col]
        nb_ref[at] = rb_ref[at, took] + p_ref[pb, half + first_col : half + last_col]


def ring_add(turn, first_col, last_col, ra, rb, partials):
    shape = (ra.shape[0], last_col - first_col)
    return pl.pallas_call(
        functools.partial(add_kernel, turn, first_col, last_col),
        name="ring_add",
        out_shape=[jax.ShapeDtypeStruct(shape, ra.dtype)] * 2,
        in_specs=[pl.BlockSpec(memory_space=pltpu.VMEM)] * 3,
        out_specs=[pl.BlockSpec(memory_space=pltpu.VMEM)] * 2,
        compiler_params=pltpu.CompilerParams(vmem_limit_bytes=16 << 20),
        cost_estimate=pl.CostEstimate(
            flops=100_000_000, bytes_accessed=12 * ra.size, transcendentals=0
        ),
    )(ra, rb, partials[TURNS[turn][0]])


def around(v, step):
    n = lax.axis_size("head")
    return lax.ppermute(v, "head", [(i, (i + step) % n) for i in range(n)])


def first_kernel(own_ref, other_ref, w_ref, a_ref, b_ref):
    core = lax.axis_index("batch")
    depth = own_ref.shape[1]
    rows, half = a_ref.shape
    mine = pl.ds(pl.multiple_of(core * depth, depth), depth)
    theirs = pl.ds(pl.multiple_of((1 - core) * depth, depth), depth)
    tile = 512
    for i, out_ref in enumerate((a_ref, b_ref)):
        own, other = own_ref[i * rows : (i + 1) * rows], other_ref[i * rows : (i + 1) * rows]

        @pl.loop(0, half // tile)
        def _(t):
            start = pl.multiple_of(t * tile, tile)
            cols = pl.ds(pl.multiple_of(i * half + t * tile, tile), tile)
            out_ref[:, pl.ds(start, tile)] = (
                jnp.dot(own, w_ref[mine, cols], preferred_element_type=jnp.float32)
                + jnp.dot(other, w_ref[theirs, cols], preferred_element_type=jnp.float32)
            ).astype(out_ref.dtype)


def first_blocks(own, other, weight):
    rows = own.shape[0] // 2
    half = weight.shape[1] // 2
    return pl.pallas_call(
        first_kernel,
        name="first_blocks",
        out_shape=[jax.ShapeDtypeStruct((rows, half), jnp.bfloat16)] * 2,
        in_specs=[pl.BlockSpec(memory_space=pltpu.VMEM)] * 3,
        out_specs=[pl.BlockSpec(memory_space=pltpu.VMEM)] * 2,
        compiler_params=pltpu.CompilerParams(vmem_limit_bytes=24 << 20),
        cost_estimate=pl.CostEstimate(
            flops=4 * rows * half * weight.shape[0], bytes_accessed=12 << 20, transcendentals=0
        ),
    )(own, other, weight)


def ring_step(turn, a, b, partial, first_col=0):
    a, b = ring_send(a, b)
    return ring_add(turn, first_col, first_col + a.shape[1], a, b, partial)


def ring_send(a, b):
    a = around(a, 1)
    b = around(b, -1)
    return a, b


def swapped(v):
    return lax.ppermute(v, "batch", [(0, 1), (1, 0)])


def on_device(queries, key_states, value_vectors, block_doc, out_weight):
    core = lax.axis_index("batch")
    first = core == 0
    q2 = queries[0].reshape(TOK, 2 * GRP * HD)
    halves_q = (q2[:, : GRP * HD], q2[:, GRP * HD :])
    by_head = jnp.moveaxis(jnp.stack([key_states[0], value_vectors[0]]), 2, 0)
    halves_kv = (by_head[0], by_head[1])
    kv_mine = jnp.where(first, halves_kv[0], halves_kv[1])
    kv_theirs = swapped(jnp.where(first, halves_kv[1], halves_kv[0]))
    q_mine = jnp.where(first, halves_q[0], halves_q[1])
    q_theirs = swapped(jnp.where(first, halves_q[1], halves_q[0]))
    doc_theirs = swapped(block_doc)

    def of(sequence, mine, theirs):
        return jnp.where(core == sequence, mine, theirs)

    def project(attended, other):
        both = jnp.where(
            first,
            jnp.concatenate([attended, other], axis=1),
            jnp.concatenate([other, attended], axis=1),
        )
        return jnp.dot(both, out_weight, preferred_element_type=jnp.float32).astype(jnp.bfloat16)

    tie = lax.optimization_barrier
    z = lax.axis_index("seq") % ZN
    units0 = gather_apart(of(0, kv_mine, kv_theirs), z)

    own1 = of(1, kv_mine, kv_theirs)
    edge1 = lax.ppermute(own1, "seq", [(ZN - 1, 0)])
    corner1 = from_corner(edge1)
    y1 = along_x(own1, 1)
    y2 = along_x(own1, 2)
    units0, (own1, y1, y2) = tie((units0, (own1, y1, y2)))
    stack1 = jnp.stack([own1, y1, y2])
    up1 = jnp.stack([jnp.where(z == 0, own1, y2), y1])
    below1 = along_z(stack1, 1)
    above1 = along_z(up1, -1)
    doc0, q0 = of(0, block_doc, doc_theirs), of(0, q_mine, q_theirs)
    early0 = attention(doc0, q0, units0, APART, 0)
    early0_other = swapped(early0)
    a0, b0 = first_blocks(early0, early0_other, out_weight)
    (q0, doc0, early0, early0_other), _ = tie(((q0, doc0, early0, early0_other), (a0, b0)))
    late0 = attention(doc0, q0, units0, APART, 1)
    late0_other = swapped(late0)
    late0_sum = project(late0, late0_other)
    early0_sum = project(early0, early0_other)
    partial0 = (early0_sum, late0_sum)

    (below1, above1), _ = tie(((below1, above1), (a0, b0)))
    far_mixed1 = along_z(jnp.where((z == 1) | (z == 2), below1[0], below1[2]), 1)
    far_x1 = along_z(above1[1], -1)
    units1 = [stack1, below1, above1, far_mixed1, far_x1, corner1]
    doc1, q1 = of(1, block_doc, doc_theirs), of(1, q_mine, q_theirs)
    a0, b0 = ring_step(0, a0, b0, partial0)
    early1 = attention(doc1, q1, units1, STACKED, 0)
    early1_other = swapped(early1)
    a1, b1 = first_blocks(early1, early1_other, out_weight)
    a0, b0 = ring_step(1, a0, b0, partial0)
    late1 = attention(doc1, q1, units1, STACKED, 1)
    a0, b0 = ring_step(2, a0, b0, partial0)
    late1_other = swapped(late1)
    (early1, early1_other), _ = tie(((early1, early1_other), (a1, b1)))
    late1_sum = project(late1, late1_other)
    early1_sum = project(early1, early1_other)
    partial1 = (early1_sum, late1_sum)
    width = a1.shape[1] // STREAMS
    a1, b1 = ring_send(a1, b1)
    tails = []
    for i in range(STREAMS):
        a, b = ring_add(0, i * width, (i + 1) * width, a1, b1, partial1)
        for turn in (1, 2):
            a, b = ring_step(turn, a, b, partial1, i * width)
        tails.append((a, b))
    sum0 = jnp.concatenate([a0, b0], axis=1)
    sum1 = jnp.concatenate([t[0] for t in tails] + [t[1] for t in tails], axis=1)
    spot = lax.broadcasted_iota(jnp.int32, (1, 2, 1), 1)
    return jnp.where(spot == 0, sum0[:, None], sum1[:, None])


def solution(mesh):
    return jax.shard_map(
        on_device,
        mesh=mesh,
        in_specs=(
            P("batch", "seq", "head", None),
            P("batch", "seq", "head", None),
            P("batch", "seq", "head", None),
            P("batch", None),
            P("head", "batch"),
        ),
        out_specs=P(("seq", "head"), None, "batch"),
        check_vma=False,
    )
```
